32 devices in a mesh: grp: 2 (over y), tx: 4 (over z), ty: 4 (over x, core).
Axes of the slice: x: 2, y: 2, z: 4, core: 2. Of those that a mesh axis runs over, the one named last changes fastest.
Arguments:
- obj_field: float32 [2, 1024, 512], P(None, ('grp', 'tx'), 'ty'), parts along dimension 1, may hold values from -6 to 6
- eigenprobes: bfloat16 [2, 32, 128, 128], P(None, 'grp'), parts along dimension 1, may hold values from -1.5 to 1.5
- weights: float32 [8, 4, 3, 16], P(('grp', 'tx'), 'ty'), parts along dimension 0, may hold values from -4 to 4
- offsets: int32 [8, 4, 3, 2], P(('grp', 'tx'), 'ty'), parts along dimension 0, may hold values from 0 to 127
- counts: int32 [8, 4], P(('grp', 'tx'), 'ty'), parts along dimension 0, may hold values from 1 to 3, as said below
- amplitudes: bfloat16 [8, 4, 3, 128, 128], P(('grp', 'tx'), 'ty'), parts along dimension 0, may hold values from 0.19921875 to 3
Outputs:
- new_object: float32 [2, 1024, 512], P(None, ('grp', 'tx'), 'ty'), parts along dimension 1
- new_eigenprobes: float32 [2, 32, 128, 128], P(None, 'grp'), parts along dimension 1
The draws below stay inside these ranges and needn't reach their ends.
There are 2 independent parts, one for each index of `grp`. The reference program is written for one: setup_inputs(seed, part) draws one part's arguments, and reference() takes and returns one part's arrays. A program takes and returns all parts, laid end to end along the dimension named above; each array names one. Nothing has to cross between parts.
Inputs may be any that keep to these rules, and one draw needn't show every extreme that they name: Every tile holds 1 to 3 positions; some tile holds exactly 3; slots from counts on are unused.
All inputs are finite; a program needn't handle non-finite values.
Results may differ from the reference program's by a relative error of at most 0.0003.
Values sent between devices are 32-bit elements; how exact they have to be, the bound alone decides.
A program may use at most 64 MiB of HBM per device.

```python
import math
import jax
import jax.numpy as jnp
from jax import lax

FRAME = 128
MODES = 16
TILE = 128
SLOTS = 3
HEIGHT = 512
WIDTH = 512
N_TX = 4
N_TY = 4


def draw_counts(key, part):
    first_key = jax.random.fold_in(key, 11)
    second_key = jax.random.fold_in(key, 12)
    spot_key = jax.random.fold_in(key, 13)
    first = jax.random.randint(first_key, (N_TX * N_TY,), 0, SLOTS)
    second = jax.random.randint(second_key, (N_TX * N_TY,), 0, SLOTS)
    loads = 1 + first * second // SLOTS
    spot = jax.random.randint(spot_key, (), 0, N_TX * N_TY)
    loads = jnp.where(jnp.arange(N_TX * N_TY) == spot, SLOTS, loads)
    return loads.reshape(N_TX, N_TY).astype(jnp.int32)


def plant(drawn, stream_key, smallest, largest):
    extent = drawn.shape
    place = [jax.random.randint(jax.random.fold_in(stream_key, axis), (), 0, extent[axis]) for axis in range(len(extent))]
    drawn = drawn.at[tuple(place)].set(smallest)
    longest = extent.index(max(extent))
    place[longest] = (place[longest] + 1) % extent[longest]
    return drawn.at[tuple(place)].set(largest)


def block_levels(stream_key, shape, shards, least, high):
    factor_of = 1.0
    for position, shards_of in shards:
        heights = jax.random.uniform(jax.random.fold_in(jax.random.fold_in(stream_key, 6), position), (shards_of,), jnp.float32, least / len(shards), high / len(shards))
        factor_of = factor_of * jnp.repeat(jnp.exp(heights), shape[position] // shards_of).reshape((-1,) + (1,) * (len(shape) - 1 - position))
    return factor_of


def scatter_about(stream_key, dims, scale, reach, split=(), kind=jnp.bfloat16):
    level = block_levels(stream_key, dims, split, -0.22, 0.18) if split else 1.0
    drawn = jax.random.normal(stream_key, dims, jnp.float32) * scale * level
    return jnp.minimum(jnp.maximum(drawn, -reach), reach).astype(kind)


def setup_inputs(seed: int = 0, part: int = 0) -> dict:
    arg_keys = jax.random.split(jax.random.key(seed), 7)
    own_keys = jax.random.split(jax.random.fold_in(arg_keys[6], part), 7)
    obj_field = scatter_about(own_keys[0], (2, HEIGHT, WIDTH), 1.0, 6.0, ((1, 4), (2, 4)), jnp.float32)
    eigenprobes = scatter_about(own_keys[1], (2, MODES, FRAME, FRAME), 0.25, 1.5)
    weights = scatter_about(own_keys[2], (N_TX, N_TY, SLOTS, MODES), 1.0, 4.0, ((0, 4), (1, 4)), jnp.float32)
    offsets = plant(jax.random.randint(own_keys[3], (N_TX, N_TY, SLOTS, 2), 0, TILE), jax.random.fold_in(own_keys[3], 1), 0, TILE - 1).astype(jnp.int32)
    counts = draw_counts(jax.random.fold_in(jax.random.fold_in(arg_keys[6], part), 71), part)
    amplitudes = jnp.clip(jnp.exp(math.log(3.0) - 2.7119641 * jax.random.uniform(own_keys[5], (N_TX, N_TY, SLOTS, FRAME, FRAME), jnp.float32) ** block_levels(own_keys[5], (N_TX, N_TY, SLOTS, FRAME, FRAME), ((0, 4), (1, 4)), -0.2, 0.2)), 0.19921875, 3.0).astype(jnp.bfloat16)
    return {"obj_field": obj_field, "eigenprobes": eigenprobes, "weights": weights, "offsets": offsets, "counts": counts, "amplitudes": amplitudes}


def reference(obj_field, eigenprobes, weights, offsets, counts, amplitudes):
    height = obj_field.shape[1]
    width = obj_field.shape[2]
    eig = eigenprobes.astype(jnp.float32)
    ocomplex = lax.complex(obj_field[0], obj_field[1])
    ecomplex = lax.complex(eig[0], eig[1])
    idx = jnp.arange(FRAME, dtype=jnp.int32)
    slot_ids = jnp.arange(SLOTS, dtype=jnp.int32)
    high = lax.Precision.HIGHEST

    def one_tile(carry, flat):
        gobj, illum, gprobe, norms = carry
        row_tile = flat // N_TY
        col_tile = flat % N_TY
        wts = weights[row_tile, col_tile]
        offs = offsets[row_tile, col_tile]
        live = (slot_ids < counts[row_tile, col_tile]).astype(obj_field.dtype)
        amps = amplitudes[row_tile, col_tile].astype(obj_field.dtype)
        rows = ((row_tile * TILE + offs[:, 0])[:, None] + idx[None, :]).astype(jnp.int32) % height
        cols = ((col_tile * TILE + offs[:, 1])[:, None] + idx[None, :]).astype(jnp.int32) % width
        win = ocomplex[rows[:, :, None], cols[:, None, :]]
        probe_re = jnp.einsum('sk,kij->sij', wts, eig[0], precision=high)
        probe_im = jnp.einsum('sk,kij->sij', wts, eig[1], precision=high)
        probe = lax.complex(probe_re, probe_im)
        spec = jnp.fft.fft2(probe * win, norm='ortho')
        mag = jnp.sqrt(jnp.real(spec) ** 2 + jnp.imag(spec) ** 2 + 0.25)
        factor = (amps / mag - 1.0) * live[:, None, None]
        chi = jnp.fft.ifft2(spec * factor, norm='ortho')
        gobj = gobj.at[rows[:, :, None], cols[:, None, :]].add(jnp.conj(probe) * chi)
        power = (probe_re ** 2 + probe_im ** 2) * live[:, None, None]
        illum = illum.at[rows[:, :, None], cols[:, None, :]].add(power)
        grad = jnp.conj(win) * chi
        add_re = jnp.einsum('sk,sij->kij', wts, jnp.real(grad), precision=high)
        add_im = jnp.einsum('sk,sij->kij', wts, jnp.imag(grad), precision=high)
        gprobe = gprobe + lax.complex(add_re, add_im)
        norms = norms + lax.optimization_barrier(jnp.sum(live[:, None] * wts * wts, axis=0))
        return ((gobj, illum, gprobe, norms), None)
    start = (jnp.zeros_like(ocomplex), jnp.zeros_like(obj_field[0]), jnp.zeros_like(ecomplex), jnp.zeros((MODES,), obj_field.dtype))
    (gobj, illum, gprobe, norms), _ = lax.scan(one_tile, start, jnp.arange(N_TX * N_TY, dtype=jnp.int32))
    mean_illum = jnp.sum(illum) / (height * width)
    new_obj = ocomplex + gobj / (illum + mean_illum)
    new_eig = ecomplex + gprobe / (norms + 1.0)[:, None, None]
    return (jnp.stack([jnp.real(new_obj), jnp.imag(new_obj)]), jnp.stack([jnp.real(new_eig), jnp.imag(new_eig)]))
```

```python
import functools
import math

import jax
import jax.numpy as jnp
import numpy as np
from jax import lax
from jax.experimental import pallas as pl
from jax.experimental.pallas import tpu as pltpu
from jax.sharding import PartitionSpec as P

MESH = pl.DeviceIdType.MESH

high = lax.Precision.HIGHEST


def from_behind(value, axis, steps):
    count = lax.axis_size(axis)
    pairs = [(source, (source + steps) % count) for source in range(count)]
    return lax.ppermute(value, axis, pairs)


def tables(frame, sign):
    grid = jnp.arange(frame, dtype=jnp.int32)
    phase = grid[:, None] * grid[None, :] % frame
    angle = phase.astype(jnp.float32) * (2.0 * math.pi / frame)
    scale = 1.0 / math.sqrt(frame)
    return (jnp.cos(angle) * scale, sign * jnp.sin(angle) * scale)


def transform(real_part, imag_part, table_re, table_im):
    left_re = jnp.einsum("jk,skl->sjl", table_re, real_part, precision=high) - jnp.einsum(
        "jk,skl->sjl", table_im, imag_part, precision=high
    )
    left_im = jnp.einsum("jk,skl->sjl", table_re, imag_part, precision=high) + jnp.einsum(
        "jk,skl->sjl", table_im, real_part, precision=high
    )
    out_re = jnp.einsum("sjk,kl->sjl", left_re, table_re, precision=high) - jnp.einsum(
        "sjk,kl->sjl", left_im, table_im, precision=high
    )
    out_im = jnp.einsum("sjk,kl->sjl", left_re, table_im, precision=high) + jnp.einsum(
        "sjk,kl->sjl", left_im, table_re, precision=high
    )
    return (out_re, out_im)


def row_divisor(norms, start, count, frame, modes):
    mode_of_row = (start + jnp.arange(count, dtype=jnp.int32)) // frame % modes
    match = mode_of_row[:, None] == jnp.arange(modes, dtype=jnp.int32)[None, :]
    return jnp.sum(jnp.where(match, norms[None, :] + 1.0, 0.0), axis=1)


def per_device(obj_field, eigenprobes, weights, offsets, counts, amplitudes):
    tile = obj_field.shape[1]
    modes = eigenprobes.shape[1]
    frame = eigenprobes.shape[2]
    slots = weights.shape[2]
    wts = weights[0, 0]
    offs = offsets[0, 0]
    live = (jnp.arange(slots, dtype=jnp.int32) < counts[0, 0]).astype(jnp.float32)
    local_norms = jnp.sum(live[:, None] * wts * wts, axis=0)
    below = from_behind(obj_field, "tx", -1)
    tall = jnp.concatenate([obj_field, below], axis=1)
    beside = from_behind(tall, "ty", -1)
    region = jnp.concatenate([tall, beside], axis=2)
    zero_index = jnp.int32(0)

    def read_window(row_start, col_start):
        return lax.dynamic_slice(region, (zero_index, row_start, col_start), (2, frame, frame))

    windows = jax.vmap(read_window)(offs[:, 0], offs[:, 1])
    win_re = windows[:, 0]
    win_im = windows[:, 1]
    eig32 = eigenprobes.astype(jnp.float32)
    probe = jnp.einsum("sk,ckij->csij", wts, eig32, precision=high)
    psi_re = probe[0] * win_re - probe[1] * win_im
    psi_im = probe[0] * win_im + probe[1] * win_re
    fwd_re, fwd_im = tables(frame, -1.0)
    spec_re, spec_im = transform(psi_re, psi_im, fwd_re, fwd_im)
    amps = amplitudes[0, 0].astype(jnp.float32)
    factor = (amps / jnp.sqrt(spec_re * spec_re + spec_im * spec_im + 0.25) - 1.0) * live[
        :, None, None
    ]
    inv_re, inv_im = tables(frame, 1.0)
    chi_re, chi_im = transform(spec_re * factor, spec_im * factor, inv_re, inv_im)
    obj_re = probe[0] * chi_re + probe[1] * chi_im
    obj_im = probe[0] * chi_im - probe[1] * chi_re
    power = (probe[0] * probe[0] + probe[1] * probe[1]) * live[:, None, None]
    pieces = jnp.stack([obj_re, obj_im, power], axis=1)

    def add_slot(slot, acc):
        row_start = offs[slot, 0]
        col_start = offs[slot, 1]
        piece = lax.dynamic_index_in_dim(pieces, slot, 0, keepdims=False)
        current = lax.dynamic_slice(acc, (zero_index, row_start, col_start), (3, frame, frame))
        return lax.dynamic_update_slice(acc, current + piece, (zero_index, row_start, col_start))

    acc = jnp.zeros((3, tile + frame, tile + frame), jnp.float32)
    acc = lax.fori_loop(0, slots, add_slot, acc)
    grad_re = win_re * chi_re + win_im * chi_im
    grad_im = win_re * chi_im - win_im * chi_re
    slot_grad = jnp.stack([grad_re, grad_im])
    spilled = from_behind(acc[:, :, tile:], "ty", 1)
    merged = acc[:, :, :tile].at[:, :, :frame].add(spilled)
    dropped = from_behind(merged[:, tile:, :], "tx", 1)
    totals = merged[:, :tile, :].at[:, :frame, :].add(dropped)
    local_illum = jnp.sum(totals[2])
    norms, illum_sum = lax.psum((local_norms, local_illum), ("tx", "ty"))
    cells = lax.axis_size("tx") * lax.axis_size("ty") * tile * tile
    mean_illum = illum_sum / cells
    new_object = obj_field + totals[:2] / (totals[2] + mean_illum)[None]
    flat_rows = 2 * modes * frame
    flat_eig = eig32.reshape(flat_rows, frame)
    gprobe = jnp.einsum("sk,csij->ckij", wts, slot_grad, precision=high)
    flat_grad = gprobe.reshape(flat_rows, frame)
    share_rows = flat_rows // (lax.axis_size("tx") * lax.axis_size("ty"))
    start = lax.axis_index(("tx", "ty")) * share_rows
    share = lax.psum_scatter(flat_grad, ("tx", "ty"), scatter_dimension=0, tiled=True)
    own = lax.dynamic_slice_in_dim(flat_eig, start, share_rows, 0)
    updated = own + share / row_divisor(norms, start, share_rows, frame, modes)[:, None]
    new_eig = lax.all_gather(updated, ("tx", "ty"), axis=0, tiled=True).reshape(
        2, modes, frame, frame
    )
    return (new_object, new_eig)


def dft_tables(frame):
    grid = np.arange(frame)
    angle = (grid[:, None] * grid[None, :] % frame) * (2.0 * math.pi / frame)
    re = np.cos(angle) / math.sqrt(frame)
    im = -np.sin(angle) / math.sqrt(frame)
    right = np.block([[re, im], [-im, re]]).astype(np.float32)
    return right, np.ascontiguousarray(right.T)


def dot(a, b):
    return jnp.dot(a, b, precision=high, preferred_element_type=jnp.float32)


def fused_kernel(
    ntx, nty, w_s, off_s, cnt_s, obj, eig, w_v, amps, tab_r, tab_l, out_obj, out_eig,
    below, right, diag, probe, win, acc, in_right, in_diag, in_below, msg, msg_all, grads, grads_all, upd,
    halo_ss, halo_rs, msg_ss, msg_rs, a2a_ss, a2a_rs, sp_ss, sp_rs, gat_ss, gat_rs,
):
    frame = eig.shape[2]
    modes = eig.shape[1]
    slots = amps.shape[0]
    n = ntx * nty
    nx = nty // 2
    share = 2 * frame // n
    unit = slots * share
    mrows = msg.shape[0]
    tx = lax.axis_index("tx")
    ty = lax.axis_index("ty")
    me = tx * nty + ty
    peers = [(a, b) for a in range(ntx) for b in range(nty) if (a, b) != (0, 0)]

    def at(a, b):
        return {"tx": lax.rem(tx + (a + ntx), ntx), "ty": lax.rem(ty + (b + nty), nty)}

    def send(src, dst, ss, rs, where):
        copy = pltpu.make_async_remote_copy(
            src_ref=src, dst_ref=dst, send_sem=ss, recv_sem=rs, device_id=where, device_id_type=MESH
        )
        copy.start()
        return copy

    barrier = pltpu.get_barrier_semaphore()
    for a, b in peers:
        pl.semaphore_signal(barrier, inc=1, device_id=at(a, b), device_id_type=MESH)
    pl.semaphore_wait(barrier, n - 1)

    halo = []
    for c in range(2):
        halo.append(send(obj.at[c], below.at[c], halo_ss.at[c], halo_rs.at[c], at(-1, 0)))
    for c in range(2):
        halo.append(send(obj.at[c], right.at[c], halo_ss.at[2 + c], halo_rs.at[2 + c], at(0, -1)))

    lives = [jnp.where(s < cnt_s[0], jnp.float32(1.0), jnp.float32(0.0)) for s in range(slots)]
    step = 32

    def probe_rows(i, total):
        rows = pl.ds(pl.multiple_of(i * step, step), step)
        parts = [[None, None] for _ in range(slots)]
        for k in range(modes):
            for c in range(2):
                e = eig[c, k, rows, :].astype(jnp.float32)
                for s in range(slots):
                    term = w_s[s * modes + k] * e
                    parts[s][c] = term if k == 0 else parts[s][c] + term
        for s in range(slots):
            probe[s, 0, rows, :] = parts[s][0]
            probe[s, 1, rows, :] = parts[s][1]
            power = (parts[s][0] * parts[s][0] + parts[s][1] * parts[s][1]) * lives[s]
            total = total + jnp.sum(power, axis=0, keepdims=True)
        return total

    total = lax.fori_loop(0, frame // step, probe_rows, jnp.zeros((1, frame), jnp.float32))

    msg[...] = jnp.zeros_like(msg)
    wv = w_v[...]
    slot_id = lax.broadcasted_iota(jnp.int32, wv.shape, 0)
    msg[0:slots, 0:modes] = wv
    msg[slots : 2 * slots, 0:modes] = jnp.where(slot_id < cnt_s[0], wv * wv, 0.0)
    msg[2 * slots : 2 * slots + 1, :] = total
    mine = pl.ds(pl.multiple_of(me * mrows, mrows), mrows)
    msg_all[mine, :] = msg[...]
    msgs = [
        send(msg, msg_all.at[mine], msg_ss.at[q], msg_rs.at[q], at(a, b)) for q, (a, b) in enumerate(peers)
    ]

    lane = lax.broadcasted_iota(jnp.int32, (frame, frame), 1)
    row = lax.broadcasted_iota(jnp.int32, (frame, frame), 0)
    starts = [(off_s[2 * s], off_s[2 * s + 1]) for s in range(slots)]

    def spread(channel, piece_of):
        quads = [None] * 4
        for s in range(slots):
            r, c = starts[s]
            moved = pltpu.roll(pltpu.roll(piece_of(s), r, 0), c, 1)
            top, left = row >= r, lane >= c
            upper = jnp.where(top, moved, 0.0)
            lower = jnp.where(top, 0.0, moved)
            cut = [
                jnp.where(left, upper, 0.0), jnp.where(left, 0.0, upper),
                jnp.where(left, lower, 0.0), jnp.where(left, 0.0, lower),
            ]
            quads = [x if q is None else q + x for q, x in zip(quads, cut)]
        for q in range(4):
            acc[q, channel] = quads[q]

    spill = [None] * 9

    def push_right(channel):
        to = at(0, 1)
        spill[channel] = send(
            acc.at[3, channel], in_diag.at[channel], sp_ss.at[channel], sp_rs.at[channel], to
        )
        k = 3 + channel
        spill[k] = send(acc.at[1, channel], in_right.at[channel], sp_ss.at[k], sp_rs.at[k], to)

    def push_down(channel):
        spill[channel].wait_recv()
        acc[2, channel] = acc[2, channel] + in_diag[channel]
        k = 6 + channel
        spill[k] = send(acc.at[2, channel], in_below.at[channel], sp_ss.at[k], sp_rs.at[k], at(1, 0))

    spread(2, lambda s: (probe[s, 0] * probe[s, 0] + probe[s, 1] * probe[s, 1]) * lives[s])

    for c in range(2):
        halo[c].wait_recv()
        halo.append(send(below.at[c], diag.at[c], halo_ss.at[4 + c], halo_rs.at[4 + c], at(0, -1)))
    push_right(2)
    for c in range(2):
        halo[2 + c].wait_recv()
    for c in range(2):
        halo[4 + c].wait_recv()

    for s in range(slots):
        r, c = starts[s]
        top, left = row >= r, lane >= c
        back_r, back_c = lax.rem(frame - r, frame), lax.rem(frame - c, frame)
        for z in range(2):
            picked = jnp.where(
                top, jnp.where(left, obj[z], right[z]), jnp.where(left, below[z], diag[z])
            )
            win[s, z] = pltpu.roll(pltpu.roll(picked, back_r, 0), back_c, 1)

    stacked = jnp.concatenate(
        [
            jnp.concatenate(
                [
                    probe[s, 0] * win[s, 0] - probe[s, 1] * win[s, 1],
                    probe[s, 0] * win[s, 1] + probe[s, 1] * win[s, 0],
                ],
                axis=1,
            )
            for s in range(slots)
        ],
        axis=0,
    )
    half = dot(stacked, tab_r[...])
    upright = jnp.concatenate(
        [
            jnp.concatenate(
                [half[s * frame : (s + 1) * frame, :frame], half[s * frame : (s + 1) * frame, frame:]], axis=0
            )
            for s in range(slots)
        ],
        axis=1,
    )
    spec = dot(tab_l[...], upright)
    scaled = []
    for s in range(slots):
        re = spec[:frame, s * frame : (s + 1) * frame]
        im = spec[frame:, s * frame : (s + 1) * frame]
        factor = (amps[s].astype(jnp.float32) / jnp.sqrt(re * re + im * im + 0.25) - 1.0) * lives[s]
        scaled.append(jnp.concatenate([re * factor, im * factor], axis=0))
    half = dot(tab_r[...], jnp.concatenate(scaled, axis=1))
    flat = jnp.concatenate(
        [
            jnp.concatenate(
                [half[:frame, s * frame : (s + 1) * frame], half[frame:, s * frame : (s + 1) * frame]], axis=1
            )
            for s in range(slots)
        ],
        axis=0,
    )
    chi = dot(flat, tab_l[...])
    chis = [
        (chi[s * frame : (s + 1) * frame, :frame], chi[s * frame : (s + 1) * frame, frame:]) for s in range(slots)
    ]

    for s in range(slots):
        chi_re, chi_im = chis[s]
        pair = (
            win[s, 0] * chi_re + win[s, 1] * chi_im,
            win[s, 0] * chi_im - win[s, 1] * chi_re,
        )
        for i in range(n):
            z, start = divmod(i * share, frame)
            at_row = (i * slots + s) * share
            grads[at_row : at_row + share, :] = pair[z][start : start + share, :]
    block = pl.ds(pl.multiple_of(me * unit, unit), unit)
    swaps = []
    for q, (a, b) in enumerate(peers):
        to = at(a, b)
        theirs = pl.ds(pl.multiple_of((to["tx"] * nty + to["ty"]) * unit, unit), unit)
        swaps.append(send(grads.at[theirs], grads_all.at[block], a2a_ss.at[q], a2a_rs.at[q], to))
    grads_all[block, :] = grads[block, :]

    spread(0, lambda s: probe[s, 0] * chis[s][0] + probe[s, 1] * chis[s][1])
    push_right(0)
    spread(1, lambda s: probe[s, 0] * chis[s][1] - probe[s, 1] * chis[s][0])
    push_right(1)
    push_down(2)
    push_down(0)
    push_down(1)

    for copy in msgs:
        copy.wait_recv()
    pick = [msg_all[pl.ds(s, n, stride=mrows), :] for s in range(2 * slots)]
    mix = jnp.concatenate(pick[:slots], axis=0).T[:modes, :]
    squares = sum(pick[slots:])
    norms = dot(squares.T[:modes, :], jnp.ones((n, frame), jnp.float32))
    inverse = 1.0 / (norms + 1.0)
    mean = jnp.sum(msg_all[pl.ds(2 * slots, n, stride=mrows), :]) / (n * frame * frame)

    for copy in swaps:
        copy.wait_recv()
    wide = jnp.concatenate(
        [
            jnp.concatenate(
                [grads_all[pl.ds(s * share + r, n, stride=unit), :] for s in range(slots)], axis=0
            )
            for r in range(share)
        ],
        axis=1,
    )
    moved = dot(mix, wide)
    for r in range(share):
        upd[pl.ds(r, modes, stride=share), :] = moved[:, r * frame : (r + 1) * frame] * inverse

    def place(i):
        flat_row = i * share
        return (flat_row // frame, pl.multiple_of(lax.rem(flat_row, frame), share))

    def rows_of(a, b):
        to = at(a, b)
        z, start = place(to["tx"] * nty + to["ty"])
        return out_eig.at[z, :, pl.ds(start, share), :]

    z, start = place(me)
    own = eig[z, :, pl.ds(start, share), :].astype(jnp.float32)
    out_eig[z, :, pl.ds(start, share), :] = own + upd[...].reshape(modes, share, frame)

    core = lax.rem(ty, 2)
    ty_of = lambda j: lax.rem(ty + 2 * j, nty)
    other = {"tx": tx, "ty": ty + 1 - 2 * core}

    def gathered(d, j):
        z, start = place(lax.rem(tx - d + ntx, ntx) * nty + lax.rem(ty - 2 * j + nty, nty))
        return out_eig.at[z, :, pl.ds(start, share), :]

    def pass_on(d, j, kind, to):
        ref = gathered(d, j)
        k = (kind * ntx + d) * nx + j
        return send(ref, ref, gat_ss.at[k], gat_rs.at[k], to)

    along = {}
    across = {}
    over = []

    def hop(ref, kind, d, j, to):
        k = (kind * ntx + d) * nx + j
        return send(ref, ref, gat_ss.at[k], gat_rs.at[k], to)

    for d in range(1, ntx):
        along[d] = hop(gathered(0, 0), 0, d, 0, at(d, 0))
    for j in range(1, nx):
        across[0, j] = hop(gathered(0, 0), 1, 0, j, at(0, 2 * j))
    over.append(hop(gathered(0, 0), 2, 0, 0, other))
    for d in range(1, ntx):
        along[d].wait_recv()
        for j in range(1, nx):
            across[d, j] = hop(gathered(d, 0), 1, d, j, at(0, 2 * j))
        over.append(hop(gathered(d, 0), 2, d, 0, other))

    for k in range(3, 9):
        spill[k].wait_recv()
    illum = acc[0, 2] + in_right[2] + in_below[2] + mean
    for c in range(2):
        out_obj[c] = obj[c] + (acc[0, c] + in_right[c] + in_below[c]) / illum

    for d in range(ntx):
        for j in range(1, nx):
            across[d, j].wait_recv()
            over.append(hop(gathered(d, j), 2, d, j, other))
    for copy in over:
        copy.wait_recv()
    for copy in halo + msgs + swaps + spill + list(along.values()) + list(across.values()) + over:
        copy.wait_send()


def per_device_fused(mesh, obj_field, eigenprobes, weights, offsets, counts, amplitudes):
    ntx, nty = mesh.shape["tx"], mesh.shape["ty"]
    n = ntx * nty
    tile, width = obj_field.shape[1:]
    _, modes, frame, _ = eigenprobes.shape
    slots = weights.shape[2]
    fits = tile == width == frame and frame % 128 == 0 and nty % 2 == 0 and n % 8 == 0
    if not (fits and (2 * frame) % (16 * n) == 0 and frame % (2 * frame // n) == 0):
        return per_device(obj_field, eigenprobes, weights, offsets, counts, amplitudes)
    share = 2 * frame // n
    mrows = -(-(2 * slots + 1) // 8) * 8
    tab_r, tab_l = dft_tables(frame)
    vmem = pl.BlockSpec(memory_space=pltpu.VMEM)
    smem = pl.BlockSpec(memory_space=pltpu.SMEM)
    nx = nty // 2
    f32 = jnp.float32
    square = (frame, frame)
    dma = pltpu.SemaphoreType.DMA
    return tuple(pl.pallas_call(
        functools.partial(fused_kernel, ntx, nty),
        out_shape=(
            jax.ShapeDtypeStruct(obj_field.shape, f32),
            jax.ShapeDtypeStruct(eigenprobes.shape, f32),
        ),
        in_specs=[smem] * 3 + [vmem] * 6,
        out_specs=(vmem, vmem),
        scratch_shapes=[
            pltpu.VMEM((2,) + square, f32),
            pltpu.VMEM((2,) + square, f32),
            pltpu.VMEM((2,) + square, f32),
            pltpu.VMEM((slots, 2) + square, f32),
            pltpu.VMEM((slots, 2) + square, f32),
            pltpu.VMEM((4, 3) + square, f32),
            pltpu.VMEM((3,) + square, f32),
            pltpu.VMEM((3,) + square, f32),
            pltpu.VMEM((3,) + square, f32),
            pltpu.VMEM((mrows, frame), f32),
            pltpu.VMEM((n * mrows, frame), f32),
            pltpu.VMEM((n * slots * share, frame), f32),
            pltpu.VMEM((n * slots * share, frame), f32),
            pltpu.VMEM((modes * share, frame), f32),
            dma((6,)), dma((6,)),
            dma((n - 1,)), dma((n - 1,)),
            dma((n - 1,)), dma((n - 1,)),
            dma((9,)), dma((9,)),
            dma((3 * ntx * nx,)), dma((3 * ntx * nx,)),
        ],
        compiler_params=pltpu.CompilerParams(collective_id=0, has_side_effects=True),
    )(
        weights.reshape(slots * modes),
        offsets.reshape(slots * 2),
        counts.reshape(1),
        obj_field,
        eigenprobes,
        weights.reshape(slots, modes),
        amplitudes.reshape((slots,) + square),
        jnp.asarray(tab_r),
        jnp.asarray(tab_l),
    ))


def solution(mesh):
    return jax.shard_map(
        functools.partial(per_device_fused, mesh),
        mesh=mesh,
        in_specs=(
            P(None, ("grp", "tx"), "ty"),
            P(None, "grp", None, None),
            P(("grp", "tx"), "ty", None, None),
            P(("grp", "tx"), "ty", None, None),
            P(("grp", "tx"), "ty"),
            P(("grp", "tx"), "ty", None, None, None),
        ),
        out_specs=(P(None, ("grp", "tx"), "ty"), P(None, "grp", None, None)),
        check_vma=False,
    )
```

```python
import functools
import math

import jax
import jax.numpy as jnp
import numpy as np
from jax import lax
from jax.experimental import pallas as pl
from jax.experimental.pallas import tpu as pltpu
from jax.sharding import PartitionSpec as P

MESH = pl.DeviceIdType.MESH

high = lax.Precision.HIGHEST


def from_behind(value, axis, steps):
    count = lax.axis_size(axis)
    pairs = [(source, (source + steps) % count) for source in range(count)]
    return lax.ppermute(value, axis, pairs)


def tables(frame, sign):
    grid = jnp.arange(frame, dtype=jnp.int32)
    phase = grid[:, None] * grid[None, :] % frame
    angle = phase.astype(jnp.float32) * (2.0 * math.pi / frame)
    scale = 1.0 / math.sqrt(frame)
    return (jnp.cos(angle) * scale, sign * jnp.sin(angle) * scale)


def transform(real_part, imag_part, table_re, table_im):
    left_re = jnp.einsum("jk,skl->sjl", table_re, real_part, precision=high) - jnp.einsum(
        "jk,skl->sjl", table_im, imag_part, precision=high
    )
    left_im = jnp.einsum("jk,skl->sjl", table_re, imag_part, precision=high) + jnp.einsum(
        "jk,skl->sjl", table_im, real_part, precision=high
    )
    out_re = jnp.einsum("sjk,kl->sjl", left_re, table_re, precision=high) - jnp.einsum(
        "sjk,kl->sjl", left_im, table_im, precision=high
    )
    out_im = jnp.einsum("sjk,kl->sjl", left_re, table_im, precision=high) + jnp.einsum(
        "sjk,kl->sjl", left_im, table_re, precision=high
    )
    return (out_re, out_im)


def row_divisor(norms, start, count, frame, modes):
    mode_of_row = (start + jnp.arange(count, dtype=jnp.int32)) // frame % modes
    match = mode_of_row[:, None] == jnp.arange(modes, dtype=jnp.int32)[None, :]
    return jnp.sum(jnp.where(match, norms[None, :] + 1.0, 0.0), axis=1)


def per_device(obj_field, eigenprobes, weights, offsets, counts, amplitudes):
    tile = obj_field.shape[1]
    modes = eigenprobes.shape[1]
    frame = eigenprobes.shape[2]
    slots = weights.shape[2]
    wts = weights[0, 0]
    offs = offsets[0, 0]
    live = (jnp.arange(slots, dtype=jnp.int32) < counts[0, 0]).astype(jnp.float32)
    local_norms = jnp.sum(live[:, None] * wts * wts, axis=0)
    below = from_behind(obj_field, "tx", -1)
    tall = jnp.concatenate([obj_field, below], axis=1)
    beside = from_behind(tall, "ty", -1)
    region = jnp.concatenate([tall, beside], axis=2)
    zero_index = jnp.int32(0)

    def read_window(row_start, col_start):
        return lax.dynamic_slice(region, (zero_index, row_start, col_start), (2, frame, frame))

    windows = jax.vmap(read_window)(offs[:, 0], offs[:, 1])
    win_re = windows[:, 0]
    win_im = windows[:, 1]
    eig32 = eigenprobes.astype(jnp.float32)
    probe = jnp.einsum("sk,ckij->csij", wts, eig32, precision=high)
    psi_re = probe[0] * win_re - probe[1] * win_im
    psi_im = probe[0] * win_im + probe[1] * win_re
    fwd_re, fwd_im = tables(frame, -1.0)
    spec_re, spec_im = transform(psi_re, psi_im, fwd_re, fwd_im)
    amps = amplitudes[0, 0].astype(jnp.float32)
    factor = (amps / jnp.sqrt(spec_re * spec_re + spec_im * spec_im + 0.25) - 1.0) * live[
        :, None, None
    ]
    inv_re, inv_im = tables(frame, 1.0)
    chi_re, chi_im = transform(spec_re * factor, spec_im * factor, inv_re, inv_im)
    obj_re = probe[0] * chi_re + probe[1] * chi_im
    obj_im = probe[0] * chi_im - probe[1] * chi_re
    power = (probe[0] * probe[0] + probe[1] * probe[1]) * live[:, None, None]
    pieces = jnp.stack([obj_re, obj_im, power], axis=1)

    def add_slot(slot, acc):
        row_start = offs[slot, 0]
        col_start = offs[slot, 1]
        piece = lax.dynamic_index_in_dim(pieces, slot, 0, keepdims=False)
        current = lax.dynamic_slice(acc, (zero_index, row_start, col_start), (3, frame, frame))
        return lax.dynamic_update_slice(acc, current + piece, (zero_index, row_start, col_start))

    acc = jnp.zeros((3, tile + frame, tile + frame), jnp.float32)
    acc = lax.fori_loop(0, slots, add_slot, acc)
    grad_re = win_re * chi_re + win_im * chi_im
    grad_im = win_re * chi_im - win_im * chi_re
    slot_grad = jnp.stack([grad_re, grad_im])
    spilled = from_behind(acc[:, :, tile:], "ty", 1)
    merged = acc[:, :, :tile].at[:, :, :frame].add(spilled)
    dropped = from_behind(merged[:, tile:, :], "tx", 1)
    totals = merged[:, :tile, :].at[:, :frame, :].add(dropped)
    local_illum = jnp.sum(totals[2])
    norms, illum_sum = lax.psum((local_norms, local_illum), ("tx", "ty"))
    cells = lax.axis_size("tx") * lax.axis_size("ty") * tile * tile
    mean_illum = illum_sum / cells
    new_object = obj_field + totals[:2] / (totals[2] + mean_illum)[None]
    flat_rows = 2 * modes * frame
    flat_eig = eig32.reshape(flat_rows, frame)
    gprobe = jnp.einsum("sk,csij->ckij", wts, slot_grad, precision=high)
    flat_grad = gprobe.reshape(flat_rows, frame)
    share_rows = flat_rows // (lax.axis_size("tx") * lax.axis_size("ty"))
    start = lax.axis_index(("tx", "ty")) * share_rows
    share = lax.psum_scatter(flat_grad, ("tx", "ty"), scatter_dimension=0, tiled=True)
    own = lax.dynamic_slice_in_dim(flat_eig, start, share_rows, 0)
    updated = own + share / row_divisor(norms, start, share_rows, frame, modes)[:, None]
    new_eig = lax.all_gather(updated, ("tx", "ty"), axis=0, tiled=True).reshape(
        2, modes, frame, frame
    )
    return (new_object, new_eig)


def dft_tables(frame):
    grid = np.arange(frame)
    angle = (grid[:, None] * grid[None, :] % frame) * (2.0 * math.pi / frame)
    re = np.cos(angle) / math.sqrt(frame)
    im = -np.sin(angle) / math.sqrt(frame)
    right = np.block([[re, im], [-im, re]]).astype(np.float32)
    return right, np.ascontiguousarray(right.T)


def dot(a, b):
    return jnp.dot(a, b, precision=high, preferred_element_type=jnp.float32)


def fused_kernel(
    ntx, nty, w_s, off_s, cnt_s, obj, eig, amps, tab_r, tab_l, out_obj, out_eig,
    below, right, diag, probe, win, acc, in_right, in_diag, in_below, msg, msg_all, grads, grads_all, upd,
    halo_ss, halo_rs, msg_ss, msg_rs, a2a_ss, a2a_rs, sp_ss, sp_rs, gat_ss, gat_rs,
):
    frame = eig.shape[2]
    modes = eig.shape[1]
    slots = amps.shape[0]
    n = ntx * nty
    nx = nty // 2
    share = 2 * frame // n
    unit = slots * share
    mrows = msg.shape[0]
    tx = lax.axis_index("tx")
    ty = lax.axis_index("ty")
    me = tx * nty + ty
    peers = [(a, b) for a in range(ntx) for b in range(nty) if (a, b) != (0, 0)]

    def at(a, b):
        return {"tx": lax.rem(tx + (a + ntx), ntx), "ty": lax.rem(ty + (b + nty), nty)}

    def send(src, dst, ss, rs, where):
        copy = pltpu.make_async_remote_copy(
            src_ref=src, dst_ref=dst, send_sem=ss, recv_sem=rs, device_id=where, device_id_type=MESH
        )
        copy.start()
        return copy

    barrier = pltpu.get_barrier_semaphore()
    for a, b in peers:
        pl.semaphore_signal(barrier, inc=1, device_id=at(a, b), device_id_type=MESH)

    lives = [jnp.where(s < cnt_s[0, 0], jnp.float32(1.0), jnp.float32(0.0)) for s in range(slots)]
    step = 32

    def probe_rows(i, total):
        rows = pl.ds(pl.multiple_of(i * step, step), step)
        parts = [[None, None] for _ in range(slots)]
        for k in range(modes):
            for c in range(2):
                e = eig[c, k, rows, :].astype(jnp.float32)
                for s in range(slots):
                    term = w_s[0, 0, s, k] * e
                    parts[s][c] = term if k == 0 else parts[s][c] + term
        for s in range(slots):
            probe[s, 0, rows, :] = parts[s][0]
            probe[s, 1, rows, :] = parts[s][1]
            power = (parts[s][0] * parts[s][0] + parts[s][1] * parts[s][1]) * lives[s]
            total = total + jnp.sum(power, axis=0, keepdims=True)
        return total

    total = lax.fori_loop(0, frame // step, probe_rows, jnp.zeros((1, frame), jnp.float32))

    pl.semaphore_wait(barrier, n - 1)
    halo = []
    for c in range(2):
        halo.append(send(obj.at[c], below.at[c], halo_ss.at[c], halo_rs.at[c], at(-1, 0)))
    for c in range(2):
        halo.append(send(obj.at[c], right.at[c], halo_ss.at[2 + c], halo_rs.at[2 + c], at(0, -1)))

    spot_row = lax.broadcasted_iota(jnp.int32, msg.shape, 0)
    spot_lane = lax.broadcasted_iota(jnp.int32, msg.shape, 1)
    table = jnp.zeros(msg.shape, jnp.float32)
    for s in range(slots):
        for k in range(modes):
            w = w_s[0, 0, s, k]
            column = jnp.where(spot_row == s, w, jnp.where(spot_row == slots + s, w * w * lives[s], 0.0))
            table = jnp.where((spot_lane == k) & (spot_row % slots == s) & (spot_row < 2 * slots), column, table)
    msg[...] = table
    msg[2 * slots : 2 * slots + 1, :] = total
    mine = pl.ds(pl.multiple_of(me * mrows, mrows), mrows)
    msg_all[mine, :] = msg[...]
    msgs = [
        send(msg, msg_all.at[mine], msg_ss.at[q], msg_rs.at[q], at(a, b)) for q, (a, b) in enumerate(peers)
    ]

    lane = lax.broadcasted_iota(jnp.int32, (frame, frame), 1)
    row = lax.broadcasted_iota(jnp.int32, (frame, frame), 0)
    starts = [(off_s[0, 0, s, 0], off_s[0, 0, s, 1]) for s in range(slots)]

    def spread(channel, piece_of):
        quads = [None] * 4
        for s in range(slots):
            r, c = starts[s]
            moved = pltpu.roll(pltpu.roll(piece_of(s), r, 0), c, 1)
            top, left = row >= r, lane >= c
            upper = jnp.where(top, moved, 0.0)
            lower = jnp.where(top, 0.0, moved)
            cut = [
                jnp.where(left, upper, 0.0), jnp.where(left, 0.0, upper),
                jnp.where(left, lower, 0.0), jnp.where(left, 0.0, lower),
            ]
            quads = [x if q is None else q + x for q, x in zip(quads, cut)]
        for q in range(4):
            acc[q, channel] = quads[q]

    spill = [None] * 9

    def push_right(channel):
        to = at(0, 1)
        spill[channel] = send(
            acc.at[3, channel], in_diag.at[channel], sp_ss.at[channel], sp_rs.at[channel], to
        )
        k = 3 + channel
        spill[k] = send(acc.at[1, channel], in_right.at[channel], sp_ss.at[k], sp_rs.at[k], to)

    def push_down(channel):
        spill[channel].wait_recv()
        acc[2, channel] = acc[2, channel] + in_diag[channel]
        k = 6 + channel
        spill[k] = send(acc.at[2, channel], in_below.at[channel], sp_ss.at[k], sp_rs.at[k], at(1, 0))

    spread(2, lambda s: (probe[s, 0] * probe[s, 0] + probe[s, 1] * probe[s, 1]) * lives[s])

    for c in range(2):
        halo[c].wait_recv()
        halo.append(send(below.at[c], diag.at[c], halo_ss.at[4 + c], halo_rs.at[4 + c], at(0, -1)))
    push_right(2)
    for c in range(2):
        halo[2 + c].wait_recv()
    for c in range(2):
        halo[4 + c].wait_recv()

    for s in range(slots):
        r, c = starts[s]
        top, left = row >= r, lane >= c
        back_r, back_c = lax.rem(frame - r, frame), lax.rem(frame - c, frame)
        for z in range(2):
            picked = jnp.where(
                top, jnp.where(left, obj[z], right[z]), jnp.where(left, below[z], diag[z])
            )
            win[s, z] = pltpu.roll(pltpu.roll(picked, back_r, 0), back_c, 1)

    stacked = jnp.concatenate(
        [
            jnp.concatenate(
                [
                    probe[s, 0] * win[s, 0] - probe[s, 1] * win[s, 1],
                    probe[s, 0] * win[s, 1] + probe[s, 1] * win[s, 0],
                ],
                axis=1,
            )
            for s in range(slots)
        ],
        axis=0,
    )
    half = dot(stacked, tab_r[...])
    upright = jnp.concatenate(
        [
            jnp.concatenate(
                [half[s * frame : (s + 1) * frame, :frame], half[s * frame : (s + 1) * frame, frame:]], axis=0
            )
            for s in range(slots)
        ],
        axis=1,
    )
    spec = dot(tab_l[...], upright)
    scaled = []
    for s in range(slots):
        re = spec[:frame, s * frame : (s + 1) * frame]
        im = spec[frame:, s * frame : (s + 1) * frame]
        factor = (amps[s].astype(jnp.float32) / jnp.sqrt(re * re + im * im + 0.25) - 1.0) * lives[s]
        scaled.append(jnp.concatenate([re * factor, im * factor], axis=0))
    half = dot(tab_r[...], jnp.concatenate(scaled, axis=1))
    flat = jnp.concatenate(
        [
            jnp.concatenate(
                [half[:frame, s * frame : (s + 1) * frame], half[frame:, s * frame : (s + 1) * frame]], axis=1
            )
            for s in range(slots)
        ],
        axis=0,
    )
    chi = dot(flat, tab_l[...])
    chis = [
        (chi[s * frame : (s + 1) * frame, :frame], chi[s * frame : (s + 1) * frame, frame:]) for s in range(slots)
    ]

    for s in range(slots):
        chi_re, chi_im = chis[s]
        pair = (
            win[s, 0] * chi_re + win[s, 1] * chi_im,
            win[s, 0] * chi_im - win[s, 1] * chi_re,
        )
        for i in range(n):
            z, start = divmod(i * share, frame)
            at_row = (i * slots + s) * share
            grads[at_row : at_row + share, :] = pair[z][start : start + share, :]
    block = pl.ds(pl.multiple_of(me * unit, unit), unit)
    swaps = []
    for q, (a, b) in enumerate(peers):
        to = at(a, b)
        theirs = pl.ds(pl.multiple_of((to["tx"] * nty + to["ty"]) * unit, unit), unit)
        swaps.append(send(grads.at[theirs], grads_all.at[block], a2a_ss.at[q], a2a_rs.at[q], to))
    grads_all[block, :] = grads[block, :]

    spread(0, lambda s: probe[s, 0] * chis[s][0] + probe[s, 1] * chis[s][1])
    push_right(0)
    spread(1, lambda s: probe[s, 0] * chis[s][1] - probe[s, 1] * chis[s][0])
    push_right(1)
    push_down(2)
    push_down(0)
    push_down(1)

    for copy in msgs:
        copy.wait_recv()
    pick = [msg_all[pl.ds(s, n, stride=mrows), :] for s in range(2 * slots)]
    mix = jnp.concatenate(pick[:slots], axis=0).T[:modes, :]
    squares = sum(pick[slots:])
    norms = dot(squares.T[:modes, :], jnp.ones((n, frame), jnp.float32))
    inverse = 1.0 / (norms + 1.0)
    mean = jnp.sum(msg_all[pl.ds(2 * slots, n, stride=mrows), :]) / (n * frame * frame)

    for copy in swaps:
        copy.wait_recv()
    wide = jnp.concatenate(
        [
            jnp.concatenate(
                [grads_all[pl.ds(s * share + r, n, stride=unit), :] for s in range(slots)], axis=0
            )
            for r in range(share)
        ],
        axis=1,
    )
    moved = dot(mix, wide)
    for r in range(share):
        upd[pl.ds(r, modes, stride=share), :] = moved[:, r * frame : (r + 1) * frame] * inverse

    def place(i):
        flat_row = i * share
        return (flat_row // frame, pl.multiple_of(lax.rem(flat_row, frame), share))

    z, start = place(me)
    own = eig[z, :, pl.ds(start, share), :].astype(jnp.float32)
    out_eig[z, :, pl.ds(start, share), :] = own + upd[...].reshape(modes, share, frame)

    core = lax.rem(ty, 2)
    other = {"tx": tx, "ty": ty + 1 - 2 * core}
    part = modes // 2
    used = []
    always = tx >= 0

    def inside(t):
        return (t >= 0) & (t < ntx)

    def hop(h, t, j, to, cond):
        z, start = place(lax.rem(t + ntx, ntx) * nty + lax.rem(ty - 2 * j + nty, nty))
        ref = out_eig.at[z, pl.ds(h * part, part), pl.ds(start, share), :]
        k = len(used)
        copy = pltpu.make_async_remote_copy(
            src_ref=ref, dst_ref=ref, send_sem=gat_ss.at[k], recv_sem=gat_rs.at[k],
            device_id=to, device_id_type=MESH,
        )
        used.append((copy, cond))
        return copy

    ways = [(w, e) for e in range(ntx - 1) for w in (1, -1)]
    kinds = [(0, 0)] + [(1, j) for j in range(nx)]
    got = {(w, e): inside(tx - w * (e + 1)) for w, e in ways}
    chain = {
        (w, e, h, j): hop(h, tx - w * e, j, at(w, 0), inside(tx - w * e) & inside(tx + w))
        for w, e in ways
        for h, j in kinds
    }
    across_own = {(h, j): hop(h, tx, 0, at(0, 2 * j), always) for h in (1, 0) for j in range(1, nx)}
    across = {
        (w, e, j): hop(0, tx - w * (e + 1), 0, at(0, 2 * j), got[w, e]) for w, e in ways for j in range(1, nx)
    }
    over_own = {(h, j): hop(h, tx, j, other, always) for h in (0, 1) for j in range(nx)}
    over = {
        (w, e, h, j): hop(h, tx - w * (e + 1), j, other, got[w, e])
        for w, e in ways
        for h in (0, 1)
        for j in range(nx)
    }

    def start_chain(h, j):
        for w in (1, -1):
            pl.when(inside(tx + w))(chain[w, 0, h, j].start)

    start_chain(1, 0)
    start_chain(0, 0)
    for h in (1, 0):
        for j in range(1, nx):
            across_own[h, j].start()
    for h in (1, 0):
        over_own[h, 0].start()
    for j in range(1, nx):
        across_own[1, j].wait_recv()
        start_chain(1, j)
        over_own[1, j].start()

    def arrive(w, e, h, j):
        chain[w, e, h, j].wait_recv()
        if e + 1 < ntx - 1:
            pl.when(inside(tx + w))(chain[w, e + 1, h, j].start)
        if h == 0:
            for k in range(1, nx):
                across[w, e, k].start()
        over[w, e, h, j].start()

    for e in range(ntx - 1):
        for h, j in [(1, 0), (0, 0)] + [(1, j) for j in range(1, nx)]:
            for w in (1, -1):
                pl.when(got[w, e])(functools.partial(arrive, w, e, h, j))
        if e == 0:
            for k in range(3, 9):
                spill[k].wait_recv()
            illum = acc[0, 2] + in_right[2] + in_below[2] + mean
            for c in range(2):
                out_obj[c] = obj[c] + (acc[0, c] + in_right[c] + in_below[c]) / illum

    def cross(w, e, j):
        across[w, e, j].wait_recv()
        over[w, e, 0, j].start()

    for j in range(1, nx):
        across_own[0, j].wait_recv()
        over_own[0, j].start()
        for w, e in ways:
            pl.when(got[w, e])(functools.partial(cross, w, e, j))
    for copy in over_own.values():
        copy.wait_recv()
    for (w, e, h, j), copy in over.items():
        pl.when(got[w, e])(copy.wait_recv)
    for copy in halo + msgs + swaps + spill:
        copy.wait_send()
    for copy, cond in used:
        if cond is always:
            copy.wait_send()
        else:
            pl.when(cond)(copy.wait_send)


def per_device_fused(mesh, obj_field, eigenprobes, weights, offsets, counts, amplitudes):
    ntx, nty = mesh.shape["tx"], mesh.shape["ty"]
    n = ntx * nty
    tile, width = obj_field.shape[1:]
    _, modes, frame, _ = eigenprobes.shape
    slots = weights.shape[2]
    hops = 2 * (ntx - 1)
    copies = hops * (1 + nty // 2) + (nty // 2 - 1) * (2 + hops) + nty * (1 + hops)
    fits = tile == width == frame and frame % 128 == 0 and nty % 2 == 0 and n % 8 == 0 and modes % 2 == 0
    if not (fits and (2 * frame) % (16 * n) == 0 and frame % (2 * frame // n) == 0):
        return per_device(obj_field, eigenprobes, weights, offsets, counts, amplitudes)
    share = 2 * frame // n
    mrows = -(-(2 * slots + 1) // 8) * 8
    tab_r, tab_l = dft_tables(frame)
    vmem = pl.BlockSpec(memory_space=pltpu.VMEM)
    smem = pl.BlockSpec(memory_space=pltpu.SMEM)
    f32 = jnp.float32
    square = (frame, frame)
    dma = pltpu.SemaphoreType.DMA
    return tuple(pl.pallas_call(
        functools.partial(fused_kernel, ntx, nty),
        out_shape=(
            pltpu.VMEM(obj_field.shape, f32),
            pltpu.VMEM(eigenprobes.shape, f32),
        ),
        in_specs=[smem] * 3 + [vmem] * 5,
        out_specs=(vmem, vmem),
        scratch_shapes=[
            pltpu.VMEM((2,) + square, f32),
            pltpu.VMEM((2,) + square, f32),
            pltpu.VMEM((2,) + square, f32),
            pltpu.VMEM((slots, 2) + square, f32),
            pltpu.VMEM((slots, 2) + square, f32),
            pltpu.VMEM((4, 3) + square, f32),
            pltpu.VMEM((3,) + square, f32),
            pltpu.VMEM((3,) + square, f32),
            pltpu.VMEM((3,) + square, f32),
            pltpu.VMEM((mrows, frame), f32),
            pltpu.VMEM((n * mrows, frame), f32),
            pltpu.VMEM((n * slots * share, frame), f32),
            pltpu.VMEM((n * slots * share, frame), f32),
            pltpu.VMEM((modes * share, frame), f32),
            dma((6,)), dma((6,)),
            dma((n - 1,)), dma((n - 1,)),
            dma((n - 1,)), dma((n - 1,)),
            dma((9,)), dma((9,)),
            dma((copies,)), dma((copies,)),
        ],
        compiler_params=pltpu.CompilerParams(collective_id=0, has_side_effects=True),
    )(
        weights,
        offsets,
        counts,
        obj_field,
        eigenprobes,
        amplitudes.reshape((slots,) + square),
        jnp.asarray(tab_r),
        jnp.asarray(tab_l),
    ))


def solution(mesh):
    return jax.shard_map(
        functools.partial(per_device_fused, mesh),
        mesh=mesh,
        in_specs=(
            P(None, ("grp", "tx"), "ty"),
            P(None, "grp", None, None),
            P(("grp", "tx"), "ty", None, None),
            P(("grp", "tx"), "ty", None, None),
            P(("grp", "tx"), "ty"),
            P(("grp", "tx"), "ty", None, None, None),
        ),
        out_specs=(P(None, ("grp", "tx"), "ty"), P(None, "grp", None, None)),
        check_vma=False,
    )
```
